32 devices in a mesh: py: 2 (over core), px: 2 (over y), pz: 2 (over x), site: 4 (over z).
Axes of the slice: x: 2, y: 2, z: 4, core: 2. Of those that a mesh axis runs over, the one named last changes fastest.
Arguments:
- density: float32 [256, 8, 128, 128], P(('site', 'py'), 'px', 'pz'), parts along dimension 0, may hold values from 0.2 to 1.8
- diffusivity: float32 [256, 8, 128, 128], P(('site', 'py'), 'px', 'pz'), parts along dimension 0, may hold values from 0.03 to 0.15
- source: float32 [256, 8, 128, 128], P(('site', 'py'), 'px', 'pz'), parts along dimension 0, may hold values from -0.2 to 0.2
Outputs:
- density_end: float32 [256, 8, 128, 128], P(('site', 'py'), 'px', 'pz'), parts along dimension 0
The draws below stay inside these ranges and needn't reach their ends.
There are 4 independent parts, one for each index of `site`. The reference program is written for one: setup_inputs(seed, part) draws one part's arguments, and reference() takes and returns one part's arrays. A program takes and returns all parts, laid end to end along the dimension named above; each array names one. Nothing has to cross between parts.
All inputs are finite; a program needn't handle non-finite values.
Results may differ from the reference program's by a relative error of at most 0.00002.
Values sent between devices are 32-bit elements; how exact they have to be, the bound alone decides.
A program may use at most 192 MiB of HBM per device.

```python
import jax
import jax.numpy as jnp
from jax import lax

GRID_J = 64
GRID_I = 8
GRID_K = 128
MEMBERS = 128
STEPS = 4


def level_of(own_key, shape, split, smallest, largest):
    level, own = 1.0, jax.random.fold_in(own_key, 6)
    for axis_at, parts in split:
        heights = jnp.exp(jax.random.uniform(jax.random.fold_in(own, axis_at), (parts,), jnp.float32, smallest / len(split), largest / len(split)))
        level = level * jnp.repeat(heights, shape[axis_at] // parts).reshape([-1 if axis == axis_at else 1 for axis in range(len(shape))])
    return level


def setup_inputs(seed: int = 0, part: int = 0) -> dict:
    streams_of = jax.random.split(jax.random.key(seed), 4)
    part_splits = jax.random.split(jax.random.fold_in(streams_of[3], part), 4)
    density = jnp.clip(0.2 + 1.5999999 * jax.random.uniform(part_splits[0], (GRID_J, GRID_I, GRID_K, MEMBERS), jnp.float32) ** level_of(part_splits[0], (GRID_J, GRID_I, GRID_K, MEMBERS), ((0, 2), (1, 2), (2, 2)), -0.2, 0.2), 0.2, 1.8)
    diffusivity = jnp.clip(0.03 + 0.120000007 * jax.random.uniform(part_splits[1], (GRID_J, GRID_I, GRID_K, MEMBERS), jnp.float32) ** level_of(part_splits[1], (GRID_J, GRID_I, GRID_K, MEMBERS), ((0, 2), (1, 2), (2, 2)), -0.2, 0.2), 0.03, 0.15)
    source = jnp.clip(jax.random.uniform(part_splits[2], (GRID_J, GRID_I, GRID_K, MEMBERS), jnp.float32, -0.2, 0.2) * level_of(part_splits[2], (GRID_J, GRID_I, GRID_K, MEMBERS), ((0, 2), (1, 2), (2, 2)), -0.4, 0.0), -0.2, 0.2)
    return {"density": density, "diffusivity": diffusivity, "source": source}


def inner_cells(values, dims):
    for dim in dims:
        values = lax.slice_in_dim(values, 1, values.shape[dim] - 1, axis=dim)
    return values


def side_cells(values, dim, start, dims):
    others = [other for other in dims if other != dim]
    values = inner_cells(values, others)
    return lax.slice_in_dim(values, start, start + values.shape[dim] - 2, axis=dim)


def advance(padded, diffusivity, source):
    middle = inner_cells(padded, (0, 1, 2))
    lower = [side_cells(padded, dim, 0, (0, 1, 2)) for dim in (0, 1, 2)]
    upper = [side_cells(padded, dim, 2, (0, 1, 2)) for dim in (0, 1, 2)]
    spread = lower[0] + upper[0] + lower[1] + upper[1] + lower[2] + upper[2] - 6.0 * middle
    return middle + diffusivity * spread + source


def reference(density, diffusivity, source):
    for step in range(STEPS):
        density = advance(jnp.pad(density, ((1, 1), (1, 1), (1, 1), (0, 0)), mode="constant"), diffusivity, source)
    return density
```

```python
import functools

import jax
import jax.numpy as jnp
from jax import lax
from jax.experimental import pallas as pl
from jax.experimental.pallas import tpu as pltpu
from jax.sharding import PartitionSpec as P

STEPS = 4
CHUNKS = 8
EDGE = 8
MESH = pl.DeviceIdType.MESH


def kernel(
    density,
    diffusivity,
    source,
    out,
    field,
    coef,
    src,
    result,
    k_out,
    k_in,
    load_sem,
    store_sem,
    i_send,
    i_recv,
    j_send,
    j_recv,
    k_send,
    k_recv,
):
    J, I, K, M = density.shape
    rows = J // CHUNKS
    cells = pl.ds(EDGE, K)

    def place(axis):
        me, count = lax.axis_index(axis), lax.axis_size(axis)
        return me, me > 0, me < count - 1

    pi, i_low, i_high = place("px")
    pj, j_low, j_high = place("py")
    pk, k_low, k_high = place("pz")
    has_low = {"px": i_low, "py": j_low, "pz": k_low}
    has_high = {"px": i_high, "py": j_high, "pz": k_high}
    me = {"px": pi, "py": pj, "pz": pk}

    def i_copy(side, step, chunk):
        at = pl.ds(chunk * rows, rows)
        padded = pl.ds(1 + chunk * rows, rows)
        if step == 0:
            face = density.at[at, (I - 1) if side == 0 else 0]
        else:
            face = field.at[step, padded, I if side == 0 else 1, cells]
        return pltpu.make_async_remote_copy(
            src_ref=face,
            dst_ref=field.at[step, padded, 0 if side == 0 else I + 1, cells],
            send_sem=i_send.at[side, step, chunk],
            recv_sem=i_recv.at[side, step, chunk],
            device_id={"px": pi + 1 if side == 0 else pi - 1},
            device_id_type=MESH,
        )

    def j_copy(side, step):
        if step == 0:
            face = density.at[(J - 1) if side == 0 else 0]
        else:
            face = field.at[step, J if side == 0 else 1, pl.ds(1, I), cells]
        return pltpu.make_async_remote_copy(
            src_ref=face,
            dst_ref=field.at[step, 0 if side == 0 else J + 1, pl.ds(1, I), cells],
            send_sem=j_send.at[side, step],
            recv_sem=j_recv.at[side, step],
            device_id={"py": pj + 1 if side == 0 else pj - 1},
            device_id_type=MESH,
        )

    def k_copy(side, step):
        return pltpu.make_async_remote_copy(
            src_ref=k_out.at[side, step],
            dst_ref=k_in.at[side, step],
            send_sem=k_send.at[side, step],
            recv_sem=k_recv.at[side, step],
            device_id={"pz": pk + 1 if side == 0 else pk - 1},
            device_id_type=MESH,
        )

    def goes(axis, side):
        return has_high[axis] if side == 0 else has_low[axis]

    def comes(axis, side):
        return has_low[axis] if side == 0 else has_high[axis]

    loads = [
        pltpu.make_async_copy(density, field.at[0, pl.ds(1, J), pl.ds(1, I), cells], load_sem.at[0]),
        pltpu.make_async_copy(diffusivity, coef, load_sem.at[1]),
        pltpu.make_async_copy(source, src, load_sem.at[2]),
    ]
    for load in loads:
        load.start()

    barrier = pltpu.get_barrier_semaphore()
    met = jnp.int32(0)
    for axis in ("px", "py", "pz"):
        for side in (0, 1):
            @pl.when(goes(axis, side))
            def _():
                pl.semaphore_signal(
                    barrier,
                    inc=1,
                    device_id={axis: me[axis] + 1 if side == 0 else me[axis] - 1},
                    device_id_type=MESH,
                )
            met = met + jnp.where(goes(axis, side), 1, 0).astype(jnp.int32)
    pl.semaphore_wait(barrier, met)

    for side in (0, 1):
        @pl.when(goes("px", side))
        def _():
            @pl.loop(0, CHUNKS)
            def _(chunk):
                i_copy(side, 0, chunk).start()

        @pl.when(goes("py", side))
        def _():
            j_copy(side, 0).start()

    for side in (0, 1):
        @pl.when(jnp.logical_not(comes("px", side)))
        def _():
            @pl.loop(0, J)
            def _(j):
                for step in range(STEPS):
                    field[step, j + 1, 0 if side == 0 else I + 1, cells, :] = jnp.zeros((K, M), jnp.float32)

        @pl.when(jnp.logical_not(comes("py", side)))
        def _():
            for step in range(STEPS):
                for i in range(I):
                    field[step, 0 if side == 0 else J + 1, i + 1, cells, :] = jnp.zeros((K, M), jnp.float32)

        @pl.when(jnp.logical_not(comes("pz", side)))
        def _():
            for step in range(STEPS):
                k_in[side, step] = jnp.zeros((J * I, M), jnp.float32)

    def pack(step, j):
        for i in range(I):
            at = pl.ds(j * I + i, 1)
            k_out[0, step, at, :] = field[step, j + 1, i + 1, pl.ds(EDGE + K - 1, 1), :]
            k_out[1, step, at, :] = field[step, j + 1, i + 1, pl.ds(EDGE, 1), :]

    loads[0].wait()

    @pl.loop(0, J)
    def _(j):
        pack(0, j)

    def start_k(step):
        for side in (0, 1):
            @pl.when(goes("pz", side))
            def _():
                k_copy(side, step).start()

    start_k(0)
    loads[1].wait()
    loads[2].wait()

    def stored(chunk):
        at = pl.ds(chunk * rows, rows)
        return pltpu.make_async_copy(result.at[at], out.at[at], store_sem.at[chunk])

    for step in range(STEPS):
        last = step == STEPS - 1
        for side in (0, 1):
            @pl.when(comes("py", side))
            def _():
                j_copy(side, step).wait_recv()

            @pl.when(comes("pz", side))
            def _():
                k_copy(side, step).wait_recv()

        @pl.loop(0, CHUNKS)
        def _(chunk):
            for side in (0, 1):
                @pl.when(comes("px", side))
                def _():
                    i_copy(side, step, chunk).wait_recv()

            @pl.loop(chunk * rows, (chunk + 1) * rows)
            def _(j):
                for i in range(I):
                    at = pl.ds(j * I + i, 1)
                    field[step, j + 1, i + 1, pl.ds(EDGE - 1, 1), :] = k_in[0, step, at, :]
                    field[step, j + 1, i + 1, pl.ds(EDGE + K, 1), :] = k_in[1, step, at, :]
                for i in range(I):
                    middle = field[step, j + 1, i + 1, cells, :]
                    spread = field[step, j, i + 1, cells, :] + field[step, j + 2, i + 1, cells, :]
                    spread = spread + field[step, j + 1, i, cells, :]
                    spread = spread + field[step, j + 1, i + 2, cells, :]
                    spread = spread + field[step, j + 1, i + 1, pl.ds(EDGE - 1, K), :]
                    spread = spread + field[step, j + 1, i + 1, pl.ds(EDGE + 1, K), :]
                    spread = spread - 6.0 * middle
                    value = middle + coef[j, i] * spread + src[j, i]
                    if last:
                        result[j, i] = value
                    else:
                        field[step + 1, j + 1, i + 1, cells, :] = value
                if not last:
                    pack(step + 1, j)

            if last:
                stored(chunk).start()
            else:
                for side in (0, 1):
                    @pl.when(goes("px", side))
                    def _():
                        i_copy(side, step + 1, chunk).start()

        if not last:
            for side in (0, 1):
                @pl.when(goes("py", side))
                def _():
                    j_copy(side, step + 1).start()
            start_k(step + 1)

    for side in (0, 1):
        @pl.when(goes("px", side))
        def _():
            for step in range(STEPS):
                @pl.loop(0, CHUNKS)
                def _(chunk):
                    i_copy(side, step, chunk).wait_send()

        @pl.when(goes("py", side))
        def _():
            for step in range(STEPS):
                j_copy(side, step).wait_send()

        @pl.when(goes("pz", side))
        def _():
            for step in range(STEPS):
                k_copy(side, step).wait_send()

    @pl.loop(0, CHUNKS)
    def _(chunk):
        stored(chunk).wait()


def body(density, diffusivity, source):
    J, I, K, M = density.shape
    f32 = jnp.float32
    any_space = pl.BlockSpec(memory_space=pl.ANY)
    dma = pltpu.SemaphoreType.DMA
    return pl.pallas_call(
        kernel,
        out_shape=jax.ShapeDtypeStruct((J, I, K, M), f32),
        in_specs=[any_space] * 3,
        out_specs=any_space,
        scratch_shapes=[
            pltpu.VMEM((STEPS, J + 2, I + 2, K + 2 * EDGE, M), f32),
            pltpu.VMEM((J, I, K, M), f32),
            pltpu.VMEM((J, I, K, M), f32),
            pltpu.VMEM((J, I, K, M), f32),
            pltpu.VMEM((2, STEPS, J * I, M), f32),
            pltpu.VMEM((2, STEPS, J * I, M), f32),
            dma((3,)),
            dma((CHUNKS,)),
            dma((2, STEPS, CHUNKS)),
            dma((2, STEPS, CHUNKS)),
            dma((2, STEPS)),
            dma((2, STEPS)),
            dma((2, STEPS)),
            dma((2, STEPS)),
        ],
        compiler_params=pltpu.CompilerParams(
            collective_id=0, has_side_effects=True, vmem_limit_bytes=60 * 1024 * 1024
        ),
    )(density, diffusivity, source)


def solution(mesh):
    placed = P(("site", "py"), "px", "pz", None)
    return jax.shard_map(body, mesh=mesh, in_specs=(placed,) * 3, out_specs=placed, check_vma=False)
```

```python
import functools

import jax
import jax.numpy as jnp
from jax import lax
from jax.experimental import pallas as pl
from jax.experimental.pallas import tpu as pltpu
from jax.sharding import PartitionSpec as P

STEPS = 4
CHUNKS = 4
SHORTEST = 2
EDGE = 8
MESH = pl.DeviceIdType.MESH


def chunks_of(J, step):
    if step < STEPS - 1:
        rows = J // CHUNKS
        return [(start, rows) for start in range(0, J, rows)]
    found, start, rows = [], 0, J // 2
    while start < J:
        found.append((start, rows))
        start += rows
        rows = max(min(rows // 2, J - start), min(SHORTEST, J - start))
    return found


def segments_of(J, step):
    cuts = {start for start, _ in chunks_of(J, step)} | {J}
    if step < STEPS - 1:
        cuts |= {start for start, _ in chunks_of(J, step + 1)}
    cuts = sorted(cuts)
    return list(zip(cuts[:-1], cuts[1:]))


def kernel(
    density,
    diffusivity,
    source,
    result,
    field,
    coef,
    src,
    k_out,
    k_in,
    load_sem,
    i_send,
    i_recv,
    j_send,
    j_recv,
    k_send,
    k_recv,
):
    J, I, K, M = density.shape
    cells = pl.ds(EDGE, K)

    def place(axis):
        me, count = lax.axis_index(axis), lax.axis_size(axis)
        return me, me > 0, me < count - 1

    pi, i_low, i_high = place("px")
    pj, j_low, j_high = place("py")
    pk, k_low, k_high = place("pz")
    has_low = {"px": i_low, "py": j_low, "pz": k_low}
    has_high = {"px": i_high, "py": j_high, "pz": k_high}
    me = {"px": pi, "py": pj, "pz": pk}

    def i_copy(side, step, chunk):
        start, rows = chunks_of(J, step)[chunk]
        padded = pl.ds(1 + start, rows)
        return pltpu.make_async_remote_copy(
            src_ref=field.at[step, padded, I if side == 0 else 1, cells],
            dst_ref=field.at[step, padded, 0 if side == 0 else I + 1, cells],
            send_sem=i_send.at[side, step, chunk],
            recv_sem=i_recv.at[side, step, chunk],
            device_id={"px": pi + 1 if side == 0 else pi - 1},
            device_id_type=MESH,
        )

    def j_copy(side, step):
        if step == 0:
            face = density.at[(J - 1) if side == 0 else 0]
        else:
            face = field.at[step, J if side == 0 else 1, pl.ds(1, I), cells]
        return pltpu.make_async_remote_copy(
            src_ref=face,
            dst_ref=field.at[step, 0 if side == 0 else J + 1, pl.ds(1, I), cells],
            send_sem=j_send.at[side, step],
            recv_sem=j_recv.at[side, step],
            device_id={"py": pj + 1 if side == 0 else pj - 1},
            device_id_type=MESH,
        )

    def k_copy(side, step):
        return pltpu.make_async_remote_copy(
            src_ref=k_out.at[side, step],
            dst_ref=k_in.at[side, step],
            send_sem=k_send.at[side, step],
            recv_sem=k_recv.at[side, step],
            device_id={"pz": pk + 1 if side == 0 else pk - 1},
            device_id_type=MESH,
        )

    def goes(axis, side):
        return has_high[axis] if side == 0 else has_low[axis]

    def comes(axis, side):
        return has_low[axis] if side == 0 else has_high[axis]

    def load(chunk):
        start, rows = chunks_of(J, 0)[chunk]
        return pltpu.make_async_copy(
            density.at[pl.ds(start, rows)],
            field.at[0, pl.ds(1 + start, rows), pl.ds(1, I), cells],
            load_sem.at[2 + chunk],
        )

    first = range(len(chunks_of(J, 0)))
    loads = [
        pltpu.make_async_copy(diffusivity, coef, load_sem.at[0]),
        pltpu.make_async_copy(source, src, load_sem.at[1]),
    ]
    for chunk in first:
        load(chunk).start()

    barrier = pltpu.get_barrier_semaphore()
    met = jnp.int32(0)
    for axis in ("px", "py", "pz"):
        for side in (0, 1):
            @pl.when(goes(axis, side))
            def _():
                pl.semaphore_signal(
                    barrier,
                    inc=1,
                    device_id={axis: me[axis] + 1 if side == 0 else me[axis] - 1},
                    device_id_type=MESH,
                )
            met = met + jnp.where(goes(axis, side), 1, 0).astype(jnp.int32)
    pl.semaphore_wait(barrier, met)

    for chunk in first:
        load(chunk).wait()
        for side in (0, 1):
            @pl.when(goes("px", side))
            def _():
                i_copy(side, 0, chunk).start()

    for side in (0, 1):
        @pl.when(goes("py", side))
        def _():
            j_copy(side, 0).start()

    for one in loads:
        one.start()

    for side in (0, 1):
        @pl.when(jnp.logical_not(comes("px", side)))
        def _():
            @pl.loop(0, J)
            def _(j):
                for step in range(STEPS):
                    field[step, j + 1, 0 if side == 0 else I + 1, cells, :] = jnp.zeros((K, M), jnp.float32)

        @pl.when(jnp.logical_not(comes("py", side)))
        def _():
            for step in range(STEPS):
                for i in range(I):
                    field[step, 0 if side == 0 else J + 1, i + 1, cells, :] = jnp.zeros((K, M), jnp.float32)

        @pl.when(jnp.logical_not(comes("pz", side)))
        def _():
            for step in range(STEPS):
                k_in[side, step] = jnp.zeros((J * I, M), jnp.float32)

    def pack(step, j):
        for i in range(I):
            at = pl.ds(j * I + i, 1)
            k_out[0, step, at, :] = field[step, j + 1, i + 1, pl.ds(EDGE + K - 1, 1), :]
            k_out[1, step, at, :] = field[step, j + 1, i + 1, pl.ds(EDGE, 1), :]

    @pl.loop(0, J)
    def _(j):
        pack(0, j)

    def start_k(step):
        for side in (0, 1):
            @pl.when(goes("pz", side))
            def _():
                k_copy(side, step).start()

    start_k(0)
    for one in loads:
        one.wait()

    for step in range(STEPS):
        last = step == STEPS - 1
        for side in (0, 1):
            @pl.when(comes("py", side))
            def _():
                j_copy(side, step).wait_recv()

            @pl.when(comes("pz", side))
            def _():
                k_copy(side, step).wait_recv()

        for begin, end in segments_of(J, step):
            for chunk, (start, _) in enumerate(chunks_of(J, step)):
                if start == begin:
                    for side in (0, 1):
                        @pl.when(comes("px", side))
                        def _():
                            i_copy(side, step, chunk).wait_recv()

            @pl.loop(begin, end)
            def _(j):
                for i in range(I):
                    at = pl.ds(j * I + i, 1)
                    field[step, j + 1, i + 1, pl.ds(EDGE - 1, 1), :] = k_in[0, step, at, :]
                    field[step, j + 1, i + 1, pl.ds(EDGE + K, 1), :] = k_in[1, step, at, :]
                for i in range(I):
                    middle = field[step, j + 1, i + 1, cells, :]
                    spread = field[step, j, i + 1, cells, :] + field[step, j + 2, i + 1, cells, :]
                    spread = spread + field[step, j + 1, i, cells, :]
                    spread = spread + field[step, j + 1, i + 2, cells, :]
                    spread = spread + field[step, j + 1, i + 1, pl.ds(EDGE - 1, K), :]
                    spread = spread + field[step, j + 1, i + 1, pl.ds(EDGE + 1, K), :]
                    spread = spread - 6.0 * middle
                    value = middle + coef[j, i] * spread + src[j, i]
                    if last:
                        result[j, i] = value
                    else:
                        field[step + 1, j + 1, i + 1, cells, :] = value
                if not last:
                    pack(step + 1, j)

            if not last:
                for chunk, (start, rows) in enumerate(chunks_of(J, step + 1)):
                    if start + rows == end:
                        for side in (0, 1):
                            @pl.when(goes("px", side))
                            def _():
                                i_copy(side, step + 1, chunk).start()

        if not last:
            for side in (0, 1):
                @pl.when(goes("py", side))
                def _():
                    j_copy(side, step + 1).start()
            start_k(step + 1)

    for side in (0, 1):
        @pl.when(goes("px", side))
        def _():
            for step in range(STEPS):
                for chunk in range(len(chunks_of(J, step))):
                    i_copy(side, step, chunk).wait_send()

        @pl.when(goes("py", side))
        def _():
            for step in range(STEPS):
                j_copy(side, step).wait_send()

        @pl.when(goes("pz", side))
        def _():
            for step in range(STEPS):
                k_copy(side, step).wait_send()


def store_kernel(result, out, sem):
    rows = result.shape[0] // CHUNKS
    copies = [
        pltpu.make_async_copy(result.at[pl.ds(c * rows, rows)], out.at[pl.ds(c * rows, rows)], sem.at[c])
        for c in range(CHUNKS)
    ]
    for copy in copies:
        copy.start()
    for copy in copies:
        copy.wait()


def body(density, diffusivity, source):
    J, I, K, M = density.shape
    f32 = jnp.float32
    copies = max(len(chunks_of(J, step)) for step in range(STEPS))
    any_space = pl.BlockSpec(memory_space=pl.ANY)
    dma = pltpu.SemaphoreType.DMA
    result = pl.pallas_call(
        kernel,
        out_shape=pltpu.VMEM((J, I, K, M), f32),
        in_specs=[any_space] * 3,
        out_specs=pl.BlockSpec(memory_space=pltpu.VMEM),
        scratch_shapes=[
            pltpu.VMEM((STEPS, J + 2, I + 2, K + 2 * EDGE, M), f32),
            pltpu.VMEM((J, I, K, M), f32),
            pltpu.VMEM((J, I, K, M), f32),
            pltpu.VMEM((2, STEPS, J * I, M), f32),
            pltpu.VMEM((2, STEPS, J * I, M), f32),
            dma((2 + CHUNKS,)),
            dma((2, STEPS, copies)),
            dma((2, STEPS, copies)),
            dma((2, STEPS)),
            dma((2, STEPS)),
            dma((2, STEPS)),
            dma((2, STEPS)),
        ],
        compiler_params=pltpu.CompilerParams(
            collective_id=0, has_side_effects=True, vmem_limit_bytes=46 * 1024 * 1024
        ),
    )(density, diffusivity, source)
    return pl.pallas_call(
        store_kernel,
        out_shape=jax.ShapeDtypeStruct((J, I, K, M), f32),
        in_specs=[pl.BlockSpec(memory_space=pltpu.VMEM)],
        out_specs=any_space,
        scratch_shapes=[dma((CHUNKS,))],
        compiler_params=pltpu.CompilerParams(vmem_limit_bytes=1024 * 1024),
    )(result)


def solution(mesh):
    placed = P(("site", "py"), "px", "pz", None)
    return jax.shard_map(body, mesh=mesh, in_specs=(placed,) * 3, out_specs=placed, check_vma=False)
```

```python
import functools

import jax
import jax.numpy as jnp
from jax import lax
from jax.experimental import pallas as pl
from jax.experimental.pallas import tpu as pltpu
from jax.sharding import PartitionSpec as P

STEPS = 4
CHUNKS = 4
SHORTEST = 2
EDGE = 8
MESH = pl.DeviceIdType.MESH


def chunks_of(J, step):
    if step < STEPS - 1:
        rows = J // CHUNKS
        return [(start, rows) for start in range(0, J, rows)]
    found, start, rows = [], 0, J // 2
    while start < J:
        found.append((start, rows))
        start += rows
        rows = max(min(rows // 2, J - start), min(SHORTEST, J - start))
    return found


def segments_of(J, step):
    cuts = {start for start, _ in chunks_of(J, step)} | {J}
    if step < STEPS - 1:
        cuts |= {start for start, _ in chunks_of(J, step + 1)}
    cuts = sorted(cuts)
    return list(zip(cuts[:-1], cuts[1:]))


def kernel(
    density,
    diffusivity,
    source,
    result,
    field,
    coef,
    src,
    k_out,
    k_in,
    load_sem,
    i_send,
    i_recv,
    j_send,
    j_recv,
    k_send,
    k_recv,
):
    J, I, K, M = density.shape
    cells = pl.ds(EDGE, K)

    def place(axis):
        me, count = lax.axis_index(axis), lax.axis_size(axis)
        return me, me > 0, me < count - 1

    pi, i_low, i_high = place("px")
    pj, j_low, j_high = place("py")
    pk, k_low, k_high = place("pz")
    has_low = {"px": i_low, "py": j_low, "pz": k_low}
    has_high = {"px": i_high, "py": j_high, "pz": k_high}
    me = {"px": pi, "py": pj, "pz": pk}

    def i_copy(side, step, chunk):
        start, rows = chunks_of(J, step)[chunk]
        padded = pl.ds(1 + start, rows)
        return pltpu.make_async_remote_copy(
            src_ref=field.at[step, padded, I if side == 0 else 1, cells],
            dst_ref=field.at[step, padded, 0 if side == 0 else I + 1, cells],
            send_sem=i_send.at[side, step, chunk],
            recv_sem=i_recv.at[side, step, chunk],
            device_id={"px": pi + 1 if side == 0 else pi - 1},
            device_id_type=MESH,
        )

    def j_copy(side, step):
        if step == 0:
            face = density.at[(J - 1) if side == 0 else 0]
        else:
            face = field.at[step, J if side == 0 else 1, pl.ds(1, I), cells]
        return pltpu.make_async_remote_copy(
            src_ref=face,
            dst_ref=field.at[step, 0 if side == 0 else J + 1, pl.ds(1, I), cells],
            send_sem=j_send.at[side, step],
            recv_sem=j_recv.at[side, step],
            device_id={"py": pj + 1 if side == 0 else pj - 1},
            device_id_type=MESH,
        )

    def k_copy(side, step):
        return pltpu.make_async_remote_copy(
            src_ref=k_out.at[side, step],
            dst_ref=k_in.at[side, step],
            send_sem=k_send.at[side, step],
            recv_sem=k_recv.at[side, step],
            device_id={"pz": pk + 1 if side == 0 else pk - 1},
            device_id_type=MESH,
        )

    def goes(axis, side):
        return has_high[axis] if side == 0 else has_low[axis]

    def comes(axis, side):
        return has_low[axis] if side == 0 else has_high[axis]

    def load(chunk, planes, count, sem):
        start, rows = chunks_of(J, 0)[chunk]
        return pltpu.make_async_copy(
            density.at[pl.ds(start, rows), pl.ds(planes, count)],
            field.at[0, pl.ds(1 + start, rows), pl.ds(1 + planes, count), cells],
            load_sem.at[sem],
        )

    faces = [load(0, 0, 1, 0), load(0, I - 1, 1, 1)]
    inner = load(0, 1, I - 2, 2)
    others = [load(chunk, 0, I, 2 + chunk) for chunk in range(1, len(chunks_of(J, 0)))]
    loads = [
        pltpu.make_async_copy(diffusivity, coef, load_sem.at[2 + CHUNKS]),
        pltpu.make_async_copy(source, src, load_sem.at[3 + CHUNKS]),
    ]

    barrier = pltpu.get_barrier_semaphore()
    met = jnp.int32(0)
    for axis in ("px", "py", "pz"):
        for side in (0, 1):
            @pl.when(goes(axis, side))
            def _():
                pl.semaphore_signal(
                    barrier,
                    inc=1,
                    device_id={axis: me[axis] + 1 if side == 0 else me[axis] - 1},
                    device_id_type=MESH,
                )
            met = met + jnp.where(goes(axis, side), 1, 0).astype(jnp.int32)
    for one in faces:
        one.start()
    pl.semaphore_wait(barrier, met)

    def start_i(chunk):
        for side in (0, 1):
            @pl.when(goes("px", side))
            def _():
                i_copy(side, 0, chunk).start()

    for one in faces:
        one.wait()
    start_i(0)
    for one in (*others, inner):
        one.start()
    for chunk, one in enumerate(others, 1):
        one.wait()
        start_i(chunk)
    inner.wait()

    for side in (0, 1):
        @pl.when(goes("py", side))
        def _():
            j_copy(side, 0).start()

    for one in loads:
        one.start()

    for side in (0, 1):
        @pl.when(jnp.logical_not(comes("px", side)))
        def _():
            @pl.loop(0, J)
            def _(j):
                for step in range(STEPS):
                    field[step, j + 1, 0 if side == 0 else I + 1, cells, :] = jnp.zeros((K, M), jnp.float32)

        @pl.when(jnp.logical_not(comes("py", side)))
        def _():
            for step in range(STEPS):
                for i in range(I):
                    field[step, 0 if side == 0 else J + 1, i + 1, cells, :] = jnp.zeros((K, M), jnp.float32)

        @pl.when(jnp.logical_not(comes("pz", side)))
        def _():
            for step in range(STEPS):
                k_in[side, step] = jnp.zeros((J * I, M), jnp.float32)

    def pack(step, j):
        for i in range(I):
            at = pl.ds(j * I + i, 1)
            k_out[0, step, at, :] = field[step, j + 1, i + 1, pl.ds(EDGE + K - 1, 1), :]
            k_out[1, step, at, :] = field[step, j + 1, i + 1, pl.ds(EDGE, 1), :]

    @pl.loop(0, J)
    def _(j):
        pack(0, j)

    def start_k(step):
        for side in (0, 1):
            @pl.when(goes("pz", side))
            def _():
                k_copy(side, step).start()

    start_k(0)
    for one in loads:
        one.wait()

    for step in range(STEPS):
        last = step == STEPS - 1
        for side in (0, 1):
            @pl.when(comes("py", side))
            def _():
                j_copy(side, step).wait_recv()

            @pl.when(comes("pz", side))
            def _():
                k_copy(side, step).wait_recv()

        for begin, end in segments_of(J, step):
            for chunk, (start, _) in enumerate(chunks_of(J, step)):
                if start == begin:
                    for side in (0, 1):
                        @pl.when(comes("px", side))
                        def _():
                            i_copy(side, step, chunk).wait_recv()

            @pl.loop(begin, end)
            def _(j):
                for i in range(I):
                    at = pl.ds(j * I + i, 1)
                    field[step, j + 1, i + 1, pl.ds(EDGE - 1, 1), :] = k_in[0, step, at, :]
                    field[step, j + 1, i + 1, pl.ds(EDGE + K, 1), :] = k_in[1, step, at, :]
                for i in range(I):
                    middle = field[step, j + 1, i + 1, cells, :]
                    spread = field[step, j, i + 1, cells, :] + field[step, j + 2, i + 1, cells, :]
                    spread = spread + field[step, j + 1, i, cells, :]
                    spread = spread + field[step, j + 1, i + 2, cells, :]
                    spread = spread + field[step, j + 1, i + 1, pl.ds(EDGE - 1, K), :]
                    spread = spread + field[step, j + 1, i + 1, pl.ds(EDGE + 1, K), :]
                    spread = spread - 6.0 * middle
                    value = middle + coef[j, i] * spread + src[j, i]
                    if last:
                        result[j, i] = value
                    else:
                        field[step + 1, j + 1, i + 1, cells, :] = value
                if not last:
                    pack(step + 1, j)

            if not last:
                for chunk, (start, rows) in enumerate(chunks_of(J, step + 1)):
                    if start + rows == end:
                        for side in (0, 1):
                            @pl.when(goes("px", side))
                            def _():
                                i_copy(side, step + 1, chunk).start()

        if not last:
            for side in (0, 1):
                @pl.when(goes("py", side))
                def _():
                    j_copy(side, step + 1).start()
            start_k(step + 1)

    for side in (0, 1):
        @pl.when(goes("px", side))
        def _():
            for step in range(STEPS):
                for chunk in range(len(chunks_of(J, step))):
                    i_copy(side, step, chunk).wait_send()

        @pl.when(goes("py", side))
        def _():
            for step in range(STEPS):
                j_copy(side, step).wait_send()

        @pl.when(goes("pz", side))
        def _():
            for step in range(STEPS):
                k_copy(side, step).wait_send()


def store_kernel(result, out, sem):
    rows = result.shape[0] // CHUNKS
    copies = [
        pltpu.make_async_copy(result.at[pl.ds(c * rows, rows)], out.at[pl.ds(c * rows, rows)], sem.at[c])
        for c in range(CHUNKS)
    ]
    for copy in copies:
        copy.start()
    for copy in copies:
        copy.wait()


def body(density, diffusivity, source):
    J, I, K, M = density.shape
    f32 = jnp.float32
    copies = max(len(chunks_of(J, step)) for step in range(STEPS))
    any_space = pl.BlockSpec(memory_space=pl.ANY)
    dma = pltpu.SemaphoreType.DMA
    result = pl.pallas_call(
        kernel,
        out_shape=pltpu.VMEM((J, I, K, M), f32),
        in_specs=[any_space] * 3,
        out_specs=pl.BlockSpec(memory_space=pltpu.VMEM),
        scratch_shapes=[
            pltpu.VMEM((STEPS, J + 2, I + 2, K + 2 * EDGE, M), f32),
            pltpu.VMEM((J, I, K, M), f32),
            pltpu.VMEM((J, I, K, M), f32),
            pltpu.VMEM((2, STEPS, J * I, M), f32),
            pltpu.VMEM((2, STEPS, J * I, M), f32),
            dma((4 + CHUNKS,)),
            dma((2, STEPS, copies)),
            dma((2, STEPS, copies)),
            dma((2, STEPS)),
            dma((2, STEPS)),
            dma((2, STEPS)),
            dma((2, STEPS)),
        ],
        compiler_params=pltpu.CompilerParams(
            collective_id=0, has_side_effects=True, vmem_limit_bytes=46 * 1024 * 1024
        ),
    )(density, diffusivity, source)
    return pl.pallas_call(
        store_kernel,
        out_shape=jax.ShapeDtypeStruct((J, I, K, M), f32),
        in_specs=[pl.BlockSpec(memory_space=pltpu.VMEM)],
        out_specs=any_space,
        scratch_shapes=[dma((CHUNKS,))],
        compiler_params=pltpu.CompilerParams(vmem_limit_bytes=1024 * 1024),
    )(result)


def solution(mesh):
    placed = P(("site", "py"), "px", "pz", None)
    return jax.shard_map(body, mesh=mesh, in_specs=(placed,) * 3, out_specs=placed, check_vma=False)
```
